512 devices in a mesh: grid: 32 (over y, x), band: 16 (over z, core).
Axes of the slice: x: 4, y: 8, z: 8, core: 2. Of those that a mesh axis runs over, the one named last changes fastest.
Arguments:
- start: float32 [1, 4, 1, 64, 32768], P(None, None, None, 'band', 'grid'), may hold values from -6 to 6
- energies: float32 [4, 64, 32768], P(None, 'band', 'grid'), may hold values from -4 to 4
- sites: int32 [3, 1], replicated, may hold values from 0 to 31
- potential: float32 [32, 32, 32], replicated, may hold values from -4 to 400
Outputs:
- alphas: float32 [1, 1, 4], replicated
- betas: float32 [1, 1, 4], replicated
- lanczos: float32 [1, 4, 1, 64, 32768], P(None, None, None, 'band', 'grid')
The draws below stay inside these ranges and needn't reach their ends.
All inputs are finite; a program needn't handle non-finite values.
Results may differ from the reference program's by a relative error of at most 0.0003.
Values sent between devices are 32-bit elements; how exact they have to be, the bound alone decides.
A program may use at most 64 MiB of HBM per device.

```python
import jax
import jax.numpy as jnp
from jax import lax

GRIDN = 32
CBANDS = 64
CORES = 4
POLS = 1
ITERS = 4
ATOMS = 1
KPOINTS = 32768


def draw_potential(key, part):
    first, second = jax.random.split(key)
    coords = jnp.arange(GRIDN, dtype=jnp.int32)
    distance = jnp.minimum(coords, GRIDN - coords).astype(jnp.float32)
    square = distance[:, None, None] ** 2 + distance[None, :, None] ** 2 + distance[None, None, :] ** 2
    radius = jnp.sqrt(square)
    spread_cells, height, tail_charge, background = (1.5, 250.0, 6.0, 3.0)
    roughness = jax.random.uniform(first, (GRIDN, GRIDN, GRIDN), jnp.float32, 0.5, 1.5)
    jitter = jax.random.uniform(second, (GRIDN, GRIDN, GRIDN), jnp.float32, -1.0, 1.0)
    peaked = height * jnp.exp(-square / (2.0 * spread_cells * spread_cells)) * roughness
    screened_tail = tail_charge / jnp.maximum(radius, 0.5)
    return peaked + screened_tail + background * jitter


def block_scale(rng, extent, shards, least, top_value):
    def one(position, parts):
        steps = jax.random.uniform(jax.random.fold_in(jax.random.fold_in(rng, 6), position), (parts,), jnp.float32, least / len(shards), top_value / len(shards))
        return jnp.repeat(jnp.exp(steps), extent[position] // parts).reshape((-1,) + (1,) * (len(extent) - position - 1))

    gain = one(*shards[0])
    for cut in shards[1:]:
        gain = gain * one(*cut)
    return gain


def scatter_about(key, extent, spread, reach, pieces=(), kind=jnp.bfloat16):
    array = spread * jax.random.normal(key, extent, jnp.float32)
    if pieces:
        array = array * block_scale(key, extent, pieces, -0.22, 0.18)
    return jnp.clip(array, -reach, reach).astype(kind)


def setup_inputs(seed: int = 0) -> dict:
    splits = jax.random.split(jax.random.key(seed), 5)
    start = scatter_about(splits[0], (ATOMS, CORES, POLS, CBANDS, KPOINTS), 1.0, 6.0, ((3, 16), (4, 32)), jnp.float32)
    energies = jnp.clip(jax.random.uniform(splits[1], (CORES, CBANDS, KPOINTS), jnp.float32, -4.0, 4.0) * block_scale(splits[1], (CORES, CBANDS, KPOINTS), ((1, 16), (2, 32)), -0.4, 0.0), -4.0, 4.0)
    sites = jax.random.randint(splits[2], (3, ATOMS), 0, GRIDN).astype(jnp.int32)
    potential = draw_potential(jax.random.fold_in(splits[4], 71), 0)
    return dict(start=start, energies=energies, sites=sites, potential=potential)


def cas_along(field_part, axis_number):
    spectrum = jnp.fft.fft(field_part, axis=axis_number)
    return (spectrum.real - spectrum.imag).astype(field_part.dtype)

def cas_three(field_part):
    return cas_along(cas_along(cas_along(field_part, 1), 2), 3)

def shift_axis(field_part, offset, axis_number):
    length = field_part.shape[axis_number]
    doubled = jnp.concatenate([field_part, field_part], axis=axis_number)
    first_index = ((length - offset) % length).astype(jnp.int32)
    return lax.dynamic_slice_in_dim(doubled, first_index, length, axis_number)

def reference(start, energies, sites, potential):
    grid_size = potential.shape[0]
    volume = grid_size * grid_size * grid_size
    shifted_list = []
    for atom_index in range(ATOMS):
        shifted = shift_axis(potential, sites[0, atom_index], 0)
        shifted = shift_axis(shifted, sites[1, atom_index], 1)
        shifted = shift_axis(shifted, sites[2, atom_index], 2)
        shifted_list.append(shifted)
    weights_all = jnp.repeat(jnp.stack(shifted_list), CORES, axis=0)

    def per_block(pair_items):
        field_block, weights = pair_items
        return cas_three(weights[None] * cas_three(field_block)) / volume

    def direct(vector):
        flat_vec = vector.reshape(ATOMS * CORES, POLS * CBANDS, grid_size, grid_size, grid_size)
        result = lax.map(per_block, (flat_vec, weights_all))
        return result.reshape(vector.shape)
    total_count = CORES * CBANDS * KPOINTS

    def inner(left, right):
        return lax.optimization_barrier(jnp.sum(left * right, axis=(1, 3, 4))) / total_count

    def expand_coef(values):
        return values[:, None, :, None, None]
    lanczos = start / expand_coef(jnp.sqrt(inner(start, start)))
    previous = jnp.zeros_like(start)
    beta_prev = jnp.zeros((ATOMS, POLS), jnp.float32)
    alpha_list = []
    beta_list = []
    for iteration in range(ITERS):
        applied = energies[None, :, None] * lanczos - direct(lanczos)
        alpha_now = inner(lanczos, applied)
        remainder = applied - expand_coef(alpha_now) * lanczos - expand_coef(beta_prev) * previous
        beta_now = jnp.sqrt(inner(remainder, remainder))
        previous = lanczos
        lanczos = remainder / expand_coef(beta_now)
        beta_prev = beta_now
        alpha_list.append(alpha_now)
        beta_list.append(beta_now)
    return (jnp.stack(alpha_list, axis=2), jnp.stack(beta_list, axis=2), lanczos)
```

```python
import functools
import math

import jax
import jax.numpy as jnp
import numpy as np
from jax import lax
from jax.experimental import pallas as pl
from jax.experimental.pallas import tpu as pltpu
from jax.sharding import PartitionSpec as P

ITERS = 4
GRIDN = 32
ROWS = GRIDN * GRIDN * GRIDN // 128
MESH = pl.DeviceIdType.MESH
F32 = jnp.float32
BF16 = jnp.bfloat16


def cas(angle):
    return np.cos(angle) + np.sin(angle)


def halves(table):
    table = jnp.asarray(table, F32)
    high = table.astype(BF16)
    return jnp.stack([high, (table - high.astype(F32)).astype(BF16)])


def tables():
    n, eight, four = np.arange(32), np.arange(8), np.arange(4)
    along = cas(2 * math.pi * np.outer(n, n) / 32)
    plus = cas(2 * math.pi * np.outer(eight, eight) / 8)
    minus = cas(-2 * math.pi * np.outer(eight, eight) / 8)
    left = np.concatenate([np.kron(along, plus), np.kron(along, minus)], axis=0)
    turn = 2 * math.pi * np.outer(four, four) / 4
    right = np.concatenate([np.kron(np.cos(turn), along), np.kron(np.sin(turn), along)], axis=0)
    angle = np.repeat(2 * math.pi * np.outer(eight, four) / 32, 32, axis=1)
    twist = np.stack([np.cos(angle), np.sin(angle)]).astype(np.float32)
    return halves(left), halves(left.T), halves(right), halves(right.T), jnp.asarray(twist)


def cut(x):
    high = x.astype(BF16)
    return high, (x - high.astype(F32)).astype(BF16)


def mm(a, b):
    return jnp.dot(a, b, preferred_element_type=F32)


def left_product(table, x):
    high, low = cut(x)
    wide = mm(table[0], jnp.concatenate([high, low], axis=1))
    return wide[:, :128] + wide[:, 128:] + mm(table[1], high)


def right_product(x, table):
    high, low = cut(x)
    return mm(high, table[0]) + mm(low, table[0]) + mm(high, table[1])


def to_spectrum(x, left, right, cosine, sine):
    both = left_product(left, x)
    a, b = both[:ROWS], both[ROWS:]
    return right_product(jnp.concatenate([cosine * a + sine * b, cosine * b - sine * a], axis=1), right)


def from_spectrum(x, left_t, right_t, cosine, sine):
    both = right_product(x, right_t)
    a, b = both[:, :128], both[:, 128:]
    return left_product(left_t, jnp.concatenate([cosine * a - sine * b, sine * a + cosine * b], axis=0))


def total(x):
    return jnp.sum(x, axis=(0, 1), keepdims=True)


def inverse(x):
    return jnp.where(x > 0.0, 1.0 / jnp.where(x > 0.0, x, 1.0), 0.0)


def kernel(
    size,
    start_ref,
    energy_ref,
    sites_ref,
    potential_ref,
    left_ref,
    left_t_ref,
    right_ref,
    right_t_ref,
    twist_ref,
    out_ref,
    alpha_ref,
    beta_ref,
    field_buf,
    energy_buf,
    doubled,
    weight_buf,
    krylov,
    basis,
    line_buf,
    plane_buf,
    field_send,
    field_recv,
    energy_send,
    energy_recv,
    basis_send,
    basis_recv,
    line_send,
    line_recv,
    plane_send,
    plane_recv,
):
    grids, bands, fields, planes, inner_total = size
    layers = bands // 2
    ratio = grids // fields
    me = lax.axis_index("grid")
    band = lax.axis_index("band")
    core = lax.rem(band, 2)
    layer = lax.div(band, 2)
    partner = band + 1 - 2 * core
    mine = lax.div(me, ratio)
    lag = lax.rem(core, ratio)
    computes = lax.rem(me, ratio) == lag
    slot = core * fields + mine

    def copy(src, dst, send, recv, grid_to, band_to):
        return pltpu.make_async_remote_copy(
            src_ref=src,
            dst_ref=dst,
            send_sem=send,
            recv_sem=recv,
            device_id={"grid": grid_to, "band": band_to},
            device_id_type=MESH,
        )

    def here(ref, send, recv):
        return copy(ref, ref, send, recv, me, band)

    barrier = pltpu.get_barrier_semaphore()

    def greet(grid_to, band_to):
        pl.semaphore_signal(
            barrier, inc=1, device_id={"grid": grid_to, "band": band_to}, device_id_type=MESH
        )

    @pl.loop(1, grids)
    def _(i):
        greet(lax.rem(me + i, grids), band)

    @pl.loop(0, grids)
    def _(i):
        greet(lax.rem(me + i, grids), partner)

    @pl.loop(1, layers)
    def _(i):
        greet(me, lax.rem(band + 2 * i, bands))

    @pl.when(computes)
    def _():
        sx, sy, sz = sites_ref[0, 0], sites_ref[1, 0], sites_ref[2, 0]
        doubled[:, 0:GRIDN, :] = potential_ref[...]
        doubled[:, GRIDN : 2 * GRIDN, :] = potential_ref[...]
        from_z = lax.broadcasted_iota(jnp.int32, (GRIDN, 128), 0)
        to_z = lax.broadcasted_iota(jnp.int32, (GRIDN, 128), 1)
        weights = jnp.zeros((ROWS, 128), F32)
        for v1 in range(4):
            first = lax.rem(8 * v1 - sy + GRIDN, GRIDN)
            rows = jnp.concatenate(
                [doubled[lax.rem(x - sx + GRIDN, GRIDN), pl.ds(first, 8), :] for x in range(GRIDN)], axis=0
            )
            lands = lax.rem(from_z + sz, GRIDN) + GRIDN * v1
            choose = jnp.where(lands == to_z, 1.0, 0.0).astype(BF16)
            high = rows.astype(BF16)
            rest = rows - high.astype(F32)
            middle = rest.astype(BF16)
            low = (rest - middle.astype(F32)).astype(BF16)
            weights = weights + (mm(high, choose) + mm(middle, choose) + mm(low, choose))
        weight_buf[...] = weights * (1.0 / (GRIDN * GRIDN * GRIDN))

    pl.semaphore_wait(barrier, 2 * grids - 1 + layers - 1)

    for src, dst, send, recv in (
        (start_ref, field_buf, field_send, field_recv),
        (energy_ref, energy_buf, energy_send, energy_recv),
    ):

        @pl.loop(1, fields)
        def _(i, src=src, dst=dst, send=send, recv=recv):
            field = lax.rem(mine + i, fields)
            copy(src.at[field], dst.at[pl.ds(me * planes, planes)], send, recv, field * ratio + lag, band).start()

        @pl.when(jnp.logical_not(computes))
        def _(src=src, dst=dst, send=send, recv=recv):
            copy(src.at[mine], dst.at[pl.ds(me * planes, planes)], send, recv, mine * ratio + lag, band).start()

        @pl.when(computes)
        def _(src=src, dst=dst):
            dst[pl.ds(me * planes, planes)] = src[mine]

    @pl.when(computes)
    def _():
        left, left_t, right, right_t = left_ref, left_t_ref, right_ref, right_t_ref
        cosine = jnp.concatenate([twist_ref[0]] * (ROWS // 8), axis=0)
        sine = jnp.concatenate([twist_ref[1]] * (ROWS // 8), axis=0)
        rest = pl.ds(0, (grids - 1) * planes)
        here(field_buf.at[rest], field_send, field_recv).wait_recv()
        vector = field_buf[...].reshape(ROWS, 128)
        square = total(vector * vector)
        now = vector * inverse(jnp.sqrt(square))
        before = None
        beta = None
        record = [square]
        betas = []
        for step in range(ITERS):
            spectrum = to_spectrum(now, left, right, cosine, sine)
            direct = from_spectrum(spectrum * weight_buf[...], left_t, right_t, cosine, sine)
            if step == 0:
                here(energy_buf.at[rest], energy_send, energy_recv).wait_recv()
            applied = energy_buf[...].reshape(ROWS, 128) * now - direct
            alpha = total(now * applied)
            remainder = applied - alpha * now
            if step:
                remainder = remainder - beta * before
            beta = jnp.sqrt(total(remainder * remainder))
            before = now
            now = remainder * inverse(beta)
            record.append(alpha)
            betas.append(beta)
            krylov[step] = now.reshape(GRIDN, 8, 128)

            @pl.loop(1, grids)
            def _(i, step=step):
                to = lax.rem(me + i, grids)
                copy(
                    krylov.at[step, pl.ds(to * planes, planes)],
                    basis.at[mine, step],
                    basis_send,
                    basis_recv,
                    to,
                    band,
                ).start()

            basis[mine, step] = krylov[step, pl.ds(me * planes, planes)]
        lanes = lax.broadcasted_iota(jnp.int32, (1, 128), 1)
        row = jnp.zeros((1, 128), F32)
        for k, value in enumerate(record + betas):
            row = jnp.where(lanes == 16 * layer + k, value, row)
        line_buf[layer] = row

        @pl.loop(1, layers)
        def _(i):
            copy(line_buf.at[layer], line_buf.at[layer], line_send, line_recv, me, lax.rem(band + 2 * i, bands)).start()

        here(line_buf.at[pl.ds(0, layers - 1)], line_send, line_recv).wait_recv()
        plane_buf[slot] = jnp.sum(line_buf[...], axis=0)

        @pl.loop(1, grids)
        def _(i):
            copy(plane_buf.at[slot], plane_buf.at[slot], plane_send, plane_recv, lax.rem(me + i, grids), band).start()

        @pl.loop(0, grids)
        def _(i):
            copy(plane_buf.at[slot], plane_buf.at[slot], plane_send, plane_recv, lax.rem(me + i, grids), partner).start()

        here(plane_buf.at[pl.ds(0, 2 * fields - 1)], plane_send, plane_recv).wait_recv()
        here(basis.at[pl.ds(0, fields - 1)], basis_send, basis_recv).wait_recv()

    @pl.when(jnp.logical_not(computes))
    def _():
        here(plane_buf, plane_send, plane_recv).wait_recv()
        here(basis, basis_send, basis_recv).wait_recv()

    gathered = plane_buf[...].reshape(2 * fields, 128)

    def coefficient(k):
        return gathered if k == 0 else pltpu.roll(gathered, 128 - k, 1)

    lanes = lax.broadcasted_iota(jnp.int32, (2 * fields, 128), 1)
    square = jnp.where(lax.rem(lanes, 16) == 0, gathered, 0.0)
    alphas = [coefficient(1 + j) for j in range(ITERS)]
    betas = [coefficient(1 + ITERS + j) for j in range(ITERS)]
    length = jnp.sqrt(square)
    now = [length / jnp.sqrt(total(square))]
    before = []
    beta = None
    alpha_row = jnp.zeros((1, ITERS), F32)
    beta_row = jnp.zeros((1, ITERS), F32)
    place = lax.broadcasted_iota(jnp.int32, (1, ITERS), 1)
    for step in range(ITERS):
        applied = []
        for i in range(step + 2):
            terms = []
            if i < len(now):
                terms.append(alphas[i] * now[i])
            if i:
                terms.append(betas[i - 1] * now[i - 1])
            if i + 1 < len(now):
                terms.append(betas[i] * now[i + 1])
            applied.append(functools.reduce(jnp.add, terms))
        alpha = total(functools.reduce(jnp.add, [a * b for a, b in zip(now, applied)]))
        remainder = []
        for i, value in enumerate(applied):
            if i < len(now):
                value = value - alpha * now[i]
            if i < len(before):
                value = value - beta * before[i]
            remainder.append(value)
        beta = jnp.sqrt(total(functools.reduce(jnp.add, [value * value for value in remainder])))
        before = now
        now = [value / beta for value in remainder]
        alpha_row = jnp.where(place == step, alpha, alpha_row)
        beta_row = jnp.where(place == step, beta, beta_row)
    alpha_ref[0] = alpha_row
    beta_ref[0] = beta_row
    now[0] = now[0] * inverse(length)
    own = lanes[:fields] == 16 * layer
    shares = []
    for value in now:
        part = jnp.where(core == 0, value[:fields], value[fields:])
        shares.append(math.sqrt(inner_total) * jnp.sum(jnp.where(own, part, 0.0), axis=1, keepdims=True))
    for f in range(fields):
        result = start_ref[f] * shares[0][f : f + 1].reshape(1, 1, 1)
        for step in range(ITERS):
            result = result + basis[f, step] * shares[1 + step][f : f + 1].reshape(1, 1, 1)
        out_ref[f] = result

    @pl.when(computes)
    def _():
        here(start_ref.at[pl.ds(0, fields - 1)], field_send, field_recv).wait_send()
        here(energy_ref.at[pl.ds(0, fields - 1)], energy_send, energy_recv).wait_send()
        here(krylov.at[:, pl.ds(0, (grids - 1) * planes)], basis_send, basis_recv).wait_send()
        here(line_buf.at[pl.ds(0, layers - 1)], line_send, line_recv).wait_send()
        here(plane_buf.at[pl.ds(0, grids - 1)], plane_send, plane_recv).wait_send()
        here(plane_buf.at[pl.ds(0, grids)], plane_send, plane_recv).wait_send()

    @pl.when(jnp.logical_not(computes))
    def _():
        here(start_ref, field_send, field_recv).wait_send()
        here(energy_ref, energy_send, energy_recv).wait_send()


def body(size, start, energies, sites, potential):
    grids, bands, fields, planes, _ = size
    slab = (fields, planes, 8, 128)
    vmem = pl.BlockSpec(memory_space=pltpu.VMEM)
    smem = pl.BlockSpec(memory_space=pltpu.SMEM)
    dma = pltpu.SemaphoreType.DMA
    out, alphas, betas = pl.pallas_call(
        functools.partial(kernel, size),
        out_shape=(
            jax.ShapeDtypeStruct(slab, F32),
            jax.ShapeDtypeStruct((1, 1, ITERS), F32),
            jax.ShapeDtypeStruct((1, 1, ITERS), F32),
        ),
        in_specs=[vmem, vmem, smem] + [vmem] * 6,
        out_specs=(vmem, vmem, vmem),
        scratch_shapes=[
            pltpu.VMEM((GRIDN, 8, 128), F32),
            pltpu.VMEM((GRIDN, 8, 128), F32),
            pltpu.VMEM((GRIDN, 2 * GRIDN, GRIDN), F32),
            pltpu.VMEM((ROWS, 128), F32),
            pltpu.VMEM((ITERS, GRIDN, 8, 128), F32),
            pltpu.VMEM((fields, ITERS, planes, 8, 128), F32),
            pltpu.VMEM((bands // 2, 1, 128), F32),
            pltpu.VMEM((2 * fields, 1, 128), F32),
        ]
        + [dma] * 10,
        compiler_params=pltpu.CompilerParams(collective_id=0, has_side_effects=True),
    )(start.reshape(slab), energies.reshape(slab), sites, potential, *tables())
    return alphas, betas, out.reshape(start.shape)


def solution(mesh):
    grids, bands = mesh.shape["grid"], mesh.shape["band"]

    def whole(start, energies, sites, potential):
        atoms, cores, pols, band_count, points = start.shape
        fields = cores * band_count // bands
        size = (grids, bands, fields, GRIDN // grids, cores * band_count * points)
        return jax.shard_map(
            functools.partial(body, size),
            mesh=mesh,
            in_specs=(P(None, None, None, "band", "grid"), P(None, "band", "grid"), P(), P()),
            out_specs=(P(), P(), P(None, None, None, "band", "grid")),
            check_vma=False,
        )(start, energies, sites, potential)

    return whole
```

```python
import functools
import math

import jax
import jax.numpy as jnp
import numpy as np
from jax import lax
from jax.experimental import pallas as pl
from jax.experimental.pallas import tpu as pltpu
from jax.sharding import PartitionSpec as P

ITERS = 4
GRIDN = 32
ROWS = GRIDN * GRIDN * GRIDN // 128
MESH = pl.DeviceIdType.MESH
F32 = jnp.float32
BF16 = jnp.bfloat16


def cas(angle):
    return np.cos(angle) + np.sin(angle)


def halves(table):
    table = jnp.asarray(table, F32)
    high = table.astype(BF16)
    return jnp.stack([high, (table - high.astype(F32)).astype(BF16)])


def tables():
    n, eight, four = np.arange(32), np.arange(8), np.arange(4)
    along = cas(2 * math.pi * np.outer(n, n) / 32)
    plus = cas(2 * math.pi * np.outer(eight, eight) / 8)
    minus = cas(-2 * math.pi * np.outer(eight, eight) / 8)
    left = np.concatenate([np.kron(along, plus), np.kron(along, minus)], axis=0)
    turn = 2 * math.pi * np.outer(four, four) / 4
    right = np.concatenate([np.kron(np.cos(turn), along), np.kron(np.sin(turn), along)], axis=0)
    angle = np.repeat(2 * math.pi * np.outer(eight, four) / 32, 32, axis=1)
    twist = np.stack([np.cos(angle), np.sin(angle)]).astype(np.float32)
    return halves(left), halves(left.T), halves(right), halves(right.T), jnp.asarray(twist)


def cut(x):
    high = x.astype(BF16)
    return high, (x - high.astype(F32)).astype(BF16)


def mm(a, b):
    return jnp.dot(a, b, preferred_element_type=F32)


def left_product(table, x):
    high, low = cut(x)
    wide = mm(table[0], jnp.concatenate([high, low], axis=1))
    return wide[:, :128] + wide[:, 128:] + mm(table[1], high)


def right_product(x, table):
    high, low = cut(x)
    return mm(high, table[0]) + mm(low, table[0]) + mm(high, table[1])


def to_spectrum(x, left, right, cosine, sine):
    both = left_product(left, x)
    a, b = both[:ROWS], both[ROWS:]
    return right_product(jnp.concatenate([cosine * a + sine * b, cosine * b - sine * a], axis=1), right)


def from_spectrum(x, left_t, right_t, cosine, sine):
    both = right_product(x, right_t)
    a, b = both[:, :128], both[:, 128:]
    return left_product(left_t, jnp.concatenate([cosine * a - sine * b, sine * a + cosine * b], axis=0))


def total(x):
    return jnp.sum(x, axis=(0, 1), keepdims=True)


def inverse(x):
    return jnp.where(x > 0.0, 1.0 / jnp.where(x > 0.0, x, 1.0), 0.0)


def exchange_kernel(
    size,
    start_ref,
    energy_ref,
    sites_ref,
    potential_ref,
    left_hbm,
    left_t_hbm,
    right_hbm,
    right_t_hbm,
    twist_hbm,
    plane_buf,
    basis,
    start_stage,
    energy_stage,
    sites_smem,
    left,
    left_t,
    right,
    right_t,
    twist,
    energy_out,
    field_buf,
    energy_buf,
    doubled,
    weight_buf,
    krylov,
    line_buf,
    local_sems,
    field_send,
    field_recv,
    energy_send,
    energy_recv,
    basis_send,
    basis_recv,
    line_send,
    line_recv,
    plane_send,
    plane_recv,
):
    grids, bands, fields, planes, band_local, _ = size
    layers = bands // 2
    ratio = grids // fields
    me = lax.axis_index("grid")
    band = lax.axis_index("band")
    core = lax.rem(band, 2)
    layer = lax.div(band, 2)
    partner = band + 1 - 2 * core
    mine = lax.div(me, ratio)
    lag = lax.rem(core, ratio)
    computes = lax.rem(me, ratio) == lag
    slot = core * fields + mine
    everyone = functools.partial(pl.loop, unroll=True)

    def copy(src, dst, send, recv, grid_to, band_to):
        return pltpu.make_async_remote_copy(
            src_ref=src,
            dst_ref=dst,
            send_sem=send,
            recv_sem=recv,
            device_id={"grid": grid_to, "band": band_to},
            device_id_type=MESH,
        )

    def here(ref, send, recv):
        return copy(ref, ref, send, recv, me, band)

    loads = [
        pltpu.make_async_copy(src, dst, local_sems.at[i])
        for i, (src, dst) in enumerate(
            [
                (start_ref, start_stage),
                (energy_ref, energy_stage),
                (sites_ref, sites_smem),
                (potential_ref, doubled.at[:, pl.ds(0, GRIDN), :]),
                (potential_ref, doubled.at[:, pl.ds(GRIDN, GRIDN), :]),
                (left_hbm, left),
                (right_hbm, right),
                (twist_hbm, twist),
                (left_t_hbm, left_t),
                (right_t_hbm, right_t),
            ]
        )
    ]
    loads[0].start()
    loads[1].start()
    barrier = pltpu.get_barrier_semaphore()

    def greet(grid_to, band_to):
        pl.semaphore_signal(
            barrier, inc=1, device_id={"grid": grid_to, "band": band_to}, device_id_type=MESH
        )

    @everyone(1, grids)
    def _(i):
        greet(lax.rem(me + i, grids), band)

    @everyone(0, grids)
    def _(i):
        greet(lax.rem(me + i, grids), partner)

    @everyone(1, layers)
    def _(i):
        greet(me, lax.rem(band + 2 * i, bands))

    @pl.when(computes)
    def _():
        for load in loads[2:]:
            load.start()

    loads[0].wait()
    loads[1].wait()
    for f in range(fields):
        first = f // band_local * (band_local * 8 * planes) + f % band_local
        rows = pl.ds(first, 8 * planes, stride=band_local)
        basis[f, 0] = start_stage[rows, :].reshape(planes, 8, 128)
        energy_out[f] = energy_stage[rows, :].reshape(planes, 8, 128)

    @pl.when(computes)
    def _():
        for load in loads[2:5]:
            load.wait()
        sx, sy, sz = sites_smem[0, 0], sites_smem[0, 1], sites_smem[0, 2]
        from_z = lax.broadcasted_iota(jnp.int32, (GRIDN, 128), 0)
        to_z = lax.broadcasted_iota(jnp.int32, (GRIDN, 128), 1)
        weights = jnp.zeros((ROWS, 128), F32)
        for v1 in range(4):
            first = lax.rem(8 * v1 - sy + GRIDN, GRIDN)
            rows = jnp.concatenate(
                [doubled[lax.rem(x - sx + GRIDN, GRIDN), pl.ds(first, 8), :] for x in range(GRIDN)], axis=0
            )
            lands = lax.rem(from_z + sz, GRIDN) + GRIDN * v1
            choose = jnp.where(lands == to_z, 1.0, 0.0).astype(BF16)
            high = rows.astype(BF16)
            rest = rows - high.astype(F32)
            middle = rest.astype(BF16)
            low = (rest - middle.astype(F32)).astype(BF16)
            weights = weights + (mm(high, choose) + mm(middle, choose) + mm(low, choose))
        weight_buf[...] = weights * (1.0 / (GRIDN * GRIDN * GRIDN))

    pl.semaphore_wait(barrier, 2 * grids - 1 + layers - 1)

    def source(src, f):
        return src.at[f, 0] if src is basis else src.at[f]

    for src, dst, send, recv in (
        (basis, field_buf, field_send, field_recv),
        (energy_out, energy_buf, energy_send, energy_recv),
    ):

        @everyone(1, fields)
        def _(i, src=src, dst=dst, send=send, recv=recv):
            field = lax.rem(mine + i, fields)
            copy(
                source(src, field), dst.at[pl.ds(me * planes, planes)], send, recv, field * ratio + lag, band
            ).start()

        @pl.when(jnp.logical_not(computes))
        def _(src=src, dst=dst, send=send, recv=recv):
            copy(
                source(src, mine), dst.at[pl.ds(me * planes, planes)], send, recv, mine * ratio + lag, band
            ).start()

    @pl.when(computes)
    def _():
        field_buf[pl.ds(me * planes, planes)] = basis[mine, 0]
        energy_buf[pl.ds(me * planes, planes)] = energy_out[mine]
        for load in loads[5:]:
            load.wait()
        others = pl.ds(0, (grids - 1) * planes)
        here(field_buf.at[others], field_send, field_recv).wait_recv()
        cosine = jnp.concatenate([twist[0]] * (ROWS // 8), axis=0)
        sine = jnp.concatenate([twist[1]] * (ROWS // 8), axis=0)
        rest = field_buf[...].reshape(ROWS, 128)
        now = before = beta = None
        alphas = []
        squares = []
        for step in range(ITERS):
            square = total(rest * rest)
            squares.append(square)
            spectrum = to_spectrum(rest, left, right, cosine, sine)
            direct = from_spectrum(spectrum * weight_buf[...], left_t, right_t, cosine, sine)
            length = jnp.sqrt(square)
            scale = inverse(length)
            if step == 0:
                here(energy_buf.at[others], energy_send, energy_recv).wait_recv()
            before, beta = now, length
            now = rest * scale
            applied = energy_buf[...].reshape(ROWS, 128) * now - direct * scale
            if step:
                applied = applied - beta * before
            alpha = total(now * applied)
            rest = applied - alpha * now
            alphas.append(alpha)
            krylov[step] = rest.reshape(GRIDN, 8, 128)

            @everyone(1, grids)
            def _(i, step=step):
                to = lax.rem(me + i, grids)
                copy(
                    krylov.at[step, pl.ds(to * planes, planes)],
                    basis.at[mine, 1 + step],
                    basis_send,
                    basis_recv,
                    to,
                    band,
                ).start()

            basis[mine, 1 + step] = krylov[step, pl.ds(me * planes, planes)]
        squares.append(total(rest * rest))
        lanes = lax.broadcasted_iota(jnp.int32, (1, 128), 1)
        row = jnp.zeros((1, 128), F32)
        for k, value in enumerate(squares + alphas):
            row = jnp.where(lanes == 16 * layer + k, value, row)
        line_buf[layer] = row

        @everyone(1, layers)
        def _(i):
            copy(
                line_buf.at[layer], line_buf.at[layer], line_send, line_recv, me, lax.rem(band + 2 * i, bands)
            ).start()

        here(line_buf.at[pl.ds(0, layers - 1)], line_send, line_recv).wait_recv()
        plane_buf[slot] = jnp.sum(line_buf[...], axis=0)

        @everyone(1, grids)
        def _(i):
            copy(
                plane_buf.at[slot], plane_buf.at[slot], plane_send, plane_recv, lax.rem(me + i, grids), band
            ).start()

        @everyone(0, grids)
        def _(i):
            copy(
                plane_buf.at[slot], plane_buf.at[slot], plane_send, plane_recv, lax.rem(me + i, grids), partner
            ).start()

        here(plane_buf.at[pl.ds(0, 2 * fields - 1)], plane_send, plane_recv).wait_recv()
        arrived = basis.at[pl.ds(0, fields - 1), pl.ds(1, ITERS)]
        here(arrived, basis_send, basis_recv).wait_recv()
        here(basis.at[pl.ds(0, fields - 1), 0], field_send, field_recv).wait_send()
        here(energy_out.at[pl.ds(0, fields - 1)], energy_send, energy_recv).wait_send()
        here(krylov.at[:, pl.ds(0, (grids - 1) * planes)], basis_send, basis_recv).wait_send()
        here(line_buf.at[pl.ds(0, layers - 1)], line_send, line_recv).wait_send()
        here(plane_buf.at[pl.ds(0, grids - 1)], plane_send, plane_recv).wait_send()
        here(plane_buf.at[pl.ds(0, grids)], plane_send, plane_recv).wait_send()

    @pl.when(jnp.logical_not(computes))
    def _():
        here(plane_buf, plane_send, plane_recv).wait_recv()
        here(basis.at[:, pl.ds(1, ITERS)], basis_send, basis_recv).wait_recv()
        here(basis.at[:, 0], field_send, field_recv).wait_send()
        here(energy_out, energy_send, energy_recv).wait_send()


def merge_kernel(size, plane_buf, basis, out_ref, alpha_ref, beta_ref):
    grids, bands, fields, planes, band_local, inner_total = size
    band = lax.axis_index("band")
    core = lax.rem(band, 2)
    layer = lax.div(band, 2)
    gathered = plane_buf[...].reshape(2 * fields, 128)
    lanes = lax.broadcasted_iota(jnp.int32, (2 * fields, 128), 1)
    valid = lax.rem(lanes, 16) == 0

    def coefficient(k):
        return jnp.where(valid, gathered if k == 0 else pltpu.roll(gathered, 128 - k, 1), 0.0)

    lengths = [jnp.sqrt(coefficient(k)) for k in range(ITERS + 1)]
    diagonal = [coefficient(1 + ITERS + k) for k in range(ITERS)]
    offs = lengths[1:]
    rest = [lengths[0]]
    before = []
    beta = None
    place = lax.broadcasted_iota(jnp.int32, (1, ITERS), 1)
    alpha_row = jnp.zeros((1, ITERS), F32)
    beta_row = jnp.zeros((1, ITERS), F32)
    for step in range(ITERS + 1):
        square = total(functools.reduce(jnp.add, [value * value for value in rest]))
        length = jnp.sqrt(square)
        scale = 1.0 / length
        if step:
            beta_row = jnp.where(place == step - 1, length, beta_row)
        if step == ITERS:
            rest = [value * scale for value in rest]
            break
        applied = []
        for i in range(step + 2):
            terms = []
            if i < len(rest):
                terms.append(diagonal[i] * rest[i])
            if i:
                terms.append(offs[i - 1] * rest[i - 1])
            if i + 1 < len(rest):
                terms.append(offs[i] * rest[i + 1])
            applied.append(functools.reduce(jnp.add, terms))
        alpha = total(functools.reduce(jnp.add, [a * b for a, b in zip(rest, applied)])) / square
        alpha_row = jnp.where(place == step, alpha, alpha_row)
        after = []
        for i, value in enumerate(applied):
            if i < len(rest):
                value = value - alpha * rest[i]
            value = value * scale
            if i < len(before):
                value = value - length * before[i]
            after.append(value)
        before = [value * scale for value in rest]
        rest = after
    alpha_ref[0] = alpha_row
    beta_ref[0] = beta_row
    own = lanes[:fields] == 16 * layer
    shares = []
    for value, length in zip(rest, lengths):
        value = value * inverse(length)
        part = jnp.where(core == 0, value[:fields], value[fields:])
        shares.append(math.sqrt(inner_total) * jnp.sum(jnp.where(own, part, 0.0), axis=1, keepdims=True))
    for f in range(fields):
        terms = [
            basis[f, k].reshape(8 * planes, 128) * shares[k][f : f + 1].reshape(1, 1) for k in range(ITERS + 1)
        ]
        first = f // band_local * (band_local * 8 * planes) + f % band_local
        out_ref[pl.ds(first, 8 * planes, stride=band_local), :] = functools.reduce(jnp.add, terms)


def body(size, start, energies, sites, potential):
    grids, bands, fields, planes, band_local, _ = size
    slabs = fields // band_local
    flat = (fields * planes * 8, 128)

    def flatten(x):
        return x.reshape(slabs, band_local, 8 * planes, 128).transpose(0, 2, 1, 3).reshape(flat)

    vmem = pl.BlockSpec(memory_space=pltpu.VMEM)
    anywhere = pl.BlockSpec(memory_space=pltpu.HBM)
    dma = pltpu.SemaphoreType.DMA
    constants = tables()
    plane_rows, basis = pl.pallas_call(
        functools.partial(exchange_kernel, size),
        out_shape=(
            pltpu.VMEM((2 * fields, 1, 128), F32),
            pltpu.VMEM((fields, ITERS + 1, planes, 8, 128), F32),
        ),
        in_specs=[anywhere] * 9,
        out_specs=(vmem, vmem),
        scratch_shapes=[
            pltpu.VMEM(flat, F32),
            pltpu.VMEM(flat, F32),
            pltpu.SMEM((1, 3), jnp.int32),
        ]
        + [pltpu.VMEM(c.shape, c.dtype) for c in constants]
        + [
            pltpu.VMEM((fields, planes, 8, 128), F32),
            pltpu.VMEM((GRIDN, 8, 128), F32),
            pltpu.VMEM((GRIDN, 8, 128), F32),
            pltpu.VMEM((GRIDN, 2 * GRIDN, GRIDN), F32),
            pltpu.VMEM((ROWS, 128), F32),
            pltpu.VMEM((ITERS, GRIDN, 8, 128), F32),
            pltpu.VMEM((bands // 2, 1, 128), F32),
            dma((10,)),
        ]
        + [dma] * 10,
        compiler_params=pltpu.CompilerParams(
            collective_id=0, has_side_effects=True, vmem_limit_bytes=60 * 1024 * 1024
        ),
    )(flatten(start), flatten(energies), sites.T, potential, *constants)
    out, alphas, betas = pl.pallas_call(
        functools.partial(merge_kernel, size),
        out_shape=(
            jax.ShapeDtypeStruct(flat, F32),
            jax.ShapeDtypeStruct((1, 1, ITERS), F32),
            jax.ShapeDtypeStruct((1, 1, ITERS), F32),
        ),
        in_specs=[vmem, vmem],
        out_specs=(vmem, vmem, vmem),
        compiler_params=pltpu.CompilerParams(vmem_limit_bytes=16 * 1024 * 1024),
    )(plane_rows, basis)
    out = out.reshape(slabs, 8 * planes, band_local, 128).transpose(0, 2, 1, 3)
    return alphas, betas, out.reshape(start.shape)


def solution(mesh):
    grids, bands = mesh.shape["grid"], mesh.shape["band"]

    def whole(start, energies, sites, potential):
        atoms, cores, pols, band_count, points = start.shape
        band_local = band_count // bands
        size = (grids, bands, cores * band_local, GRIDN // grids, band_local, cores * band_count * points)
        return jax.shard_map(
            functools.partial(body, size),
            mesh=mesh,
            in_specs=(P(None, None, None, "band", "grid"), P(None, "band", "grid"), P(), P()),
            out_specs=(P(), P(), P(None, None, None, "band", "grid")),
            check_vma=False,
        )(start, energies, sites, potential)

    return whole
```
